32 devices in a mesh: seq: 16 (over z, y, core), exp: 2 (over x).
Axes of the slice: x: 2, y: 2, z: 4, core: 2. Of those that a mesh axis runs over, the one named last changes fastest.
Arguments:
- hidden_in: bfloat16 [6, 6144], P('exp', 'seq'), may hold values from -2 to 2
- queries: bfloat16 [6, 6144], P(None, 'exp'), may hold values from -40 to 40
- key_cache: bfloat16 [6, 8192, 1024], P(None, 'seq', 'exp'), may hold values from -16 to 16
- value_cache: bfloat16 [6, 8192, 1024], P(None, 'seq', 'exp'), may hold values from -6 to 6
- lengths: int32 [6], replicated, may hold values from 2 to 8192
- out_weight: bfloat16 [6144, 6144], P('exp', 'seq'), may hold values from -0.078125 to 0.078125
- norm_gain: float32 [6144], P('seq'), may hold values from 0.1 to 1.9
- router: bfloat16 [6144, 8], P('seq'), may hold values from -0.078125 to 0.078125
- expert_ids: int32 [6, 2], P('exp'), may hold values from 0 to 7, as said below
- capacity: int32 [8], replicated, may hold values from 1 to 3, as said below
- w_gate: bfloat16 [8, 6144, 8192], P('exp', None, 'seq'), may hold values from -0.078125 to 0.078125
- w_up: bfloat16 [8, 6144, 8192], P('exp', None, 'seq'), may hold values from -0.078125 to 0.078125
- w_down: bfloat16 [8, 8192, 6144], P('exp', 'seq'), may hold values from -0.09375 to 0.09375
Outputs:
- layer_out: bfloat16 [6, 6144], P('exp', 'seq')
The draws below stay inside these ranges and needn't reach their ends.
Inputs may be any that keep to these rules, and one draw needn't show every extreme that they name: lengths[b] counts sequence b's live cache positions, the newest token's included. `expert_ids`: the two experts of a token differ. One expert is named by every token; any other expert is named at most 3 times within one aligned block of 3 tokens. The expert that every token names has capacity 3.
All inputs are finite; a program needn't handle non-finite values.
Results may differ from the reference program's by a relative error of at most 0.0085.
Values may be sent and summed in bfloat16 or wider, within the bound.
A program may use at most 128 MiB of HBM per device.

```python
import math
import jax
import jax.numpy as jnp
from jax import lax

D = 6144
HEADS = 48
KV_HEADS = 8
HEAD_DIM = 128
EXPERTS = 8
FF_W = 8192
TOK_DEV = 3
LENGTH = 8192
SEQS = 6


def hot_expert(key):
    return jax.random.randint(jax.random.fold_in(key, 11), (), 0, EXPERTS)


def draw_expert_ids(key, part):
    favored = hot_expert(key)
    offsets = jax.random.randint(jax.random.fold_in(key, 12), (SEQS,), 1, EXPERTS)
    other_ids = (favored + offsets) % EXPERTS
    flipped = jax.random.randint(jax.random.fold_in(key, 13), (SEQS,), 0, 2)
    first_ids = jnp.where(flipped == 1, other_ids, favored)
    second_ids = jnp.where(flipped == 1, favored, other_ids)
    return jnp.stack([first_ids, second_ids], axis=1).astype(jnp.int32)


def draw_capacity(key, part):
    favored = hot_expert(key)
    limits = jax.random.randint(jax.random.fold_in(key, 14), (EXPERTS,), 1, TOK_DEV + 1)
    return jnp.where(jnp.arange(EXPERTS) == favored, TOK_DEV, limits).astype(jnp.int32)


def draw_queries(key, part):
    return jnp.clip(2.5 * jax.random.normal(jax.random.fold_in(key, 32), (SEQS, HEADS * HEAD_DIM), jnp.float32), -15.0, 15.0).astype(jnp.bfloat16)


def draw_key_cache(key, part):
    key_rows = jnp.clip(jax.random.normal(jax.random.fold_in(key, 33), (SEQS, LENGTH, KV_HEADS * HEAD_DIM), jnp.float32), -6.0, 6.0)
    return key_rows.astype(jnp.bfloat16)


def touch_ends(values, rng, least, largest):
    extent = values.shape
    place = [jax.random.randint(jax.random.fold_in(rng, axis), (), 0, extent[axis]) for axis in range(len(extent))]
    values = values.at[tuple(place)].set(least)
    longest = extent.index(max(extent))
    place[longest] = (place[longest] + 1) % extent[longest]
    return values.at[tuple(place)].set(largest)


def spiked(result, stream_key, source, target, parts, factor):
    def block_of(axis_at):
        return (jnp.arange(result.shape[axis_at]) // (result.shape[axis_at] // parts)).reshape((-1,) + (1,) * (result.ndim - 1 - axis_at))

    near = jax.random.permutation(stream_key, parts)[block_of(target)]
    second = (block_of(target) + parts // 2) % parts
    return jnp.where((block_of(source) == near) | (block_of(source) == second), factor * result, result)


def level_of(own_key, shape, split, smallest, largest):
    level = 1.0
    for axis_at, shards_of in split:
        draws = jax.random.uniform(jax.random.fold_in(jax.random.fold_in(own_key, 6), axis_at), (shards_of,), jnp.float32, smallest / len(split), largest / len(split))
        level = level * jnp.repeat(jnp.exp(draws), shape[axis_at] // shards_of).reshape((-1,) + (1,) * (len(shape) - 1 - axis_at))
    return level


def centred(own_key, dims, scale, most, shards=(), held_as=jnp.bfloat16):
    drawn = scale * jax.random.normal(own_key, dims, jnp.float32)
    if shards:
        drawn = drawn * level_of(own_key, dims, shards, -0.22, 0.18)
    return jnp.clip(drawn, -most, most).astype(held_as)


def heavy_noise(own_key, extent, width, limit, shards, heavy, kind=jnp.bfloat16):
    array = width * jax.random.normal(own_key, extent, jnp.float32)
    if shards:
        array = array * level_of(own_key, extent, shards, -0.22, 0.18)
    return jnp.clip(spiked(array, jax.random.fold_in(own_key, 3), *heavy), -limit, limit).astype(kind)


def setup_inputs(seed: int = 0) -> dict:
    arg_keys = jax.random.split(jax.random.key(seed), 14)
    return {
        "hidden_in": centred(arg_keys[0], (SEQS, D), 0.3, 2.0, ((0, 2), (1, 16))),
        "queries": draw_queries(jax.random.fold_in(arg_keys[13], 71), 0),
        "key_cache": draw_key_cache(jax.random.fold_in(arg_keys[13], 71), 0),
        "value_cache": centred(arg_keys[3], (SEQS, LENGTH, KV_HEADS * HEAD_DIM), 1.0, 6.0, ((1, 16), (2, 2))),
        "lengths": touch_ends(jax.random.randint(arg_keys[4], (SEQS,), 2, LENGTH + 1), jax.random.fold_in(arg_keys[4], 1), 2, LENGTH).astype(jnp.int32),
        "out_weight": centred(arg_keys[5], (HEADS * HEAD_DIM, D), (HEADS * HEAD_DIM) ** -0.5, 0.078125, ((0, 2), (1, 16))),
        "norm_gain": jnp.clip(1.0 + 0.18 * jax.random.normal(arg_keys[6], (D,), jnp.float32), 0.1, 1.9),
        "router": centred(arg_keys[7], (D, EXPERTS), D ** -0.5, 0.078125, ((0, 16),)),
        "expert_ids": draw_expert_ids(jax.random.fold_in(arg_keys[13], 71), 0),
        "capacity": draw_capacity(jax.random.fold_in(arg_keys[13], 71), 0),
        "w_gate": centred(arg_keys[10], (EXPERTS, D, FF_W), D ** -0.5, 0.078125, ((0, 2), (2, 16))),
        "w_up": centred(arg_keys[11], (EXPERTS, D, FF_W), D ** -0.5, 0.078125, ((0, 2), (2, 16))),
        "w_down": heavy_noise(arg_keys[12], (EXPERTS, FF_W, D), FF_W ** -0.5, 0.09375, ((0, 2), (1, 16)), (1, 2, 16, 2.0)),
    }


masked_score = -1e+30
norm_eps = 1e-05

def expert_rows(normed, gate_mat, up_mat, down_weight_matrix):
    gate_sum = jnp.dot(normed, gate_mat, preferred_element_type=jnp.float32)
    up_sum = jnp.dot(normed, up_mat, preferred_element_type=jnp.float32)
    hidden_act = (jax.nn.silu(gate_sum) * up_sum).astype(jnp.bfloat16)
    return jnp.dot(hidden_act, down_weight_matrix, preferred_element_type=jnp.float32)

def reference(hidden_in, queries, key_cache, value_cache, lengths, out_weight, norm_gain, router, expert_ids, capacity, w_gate, w_up, w_down):
    group_size = HEADS // KV_HEADS
    query_heads = queries.astype(jnp.float32).reshape(SEQS, KV_HEADS, group_size, HEAD_DIM)
    positions = jnp.arange(LENGTH, dtype=jnp.int32)
    live_mask = positions[None, :] < lengths[:, None]
    outputs = []
    for kv_index in range(KV_HEADS):
        key_rows = key_cache[:, :, kv_index * HEAD_DIM:(kv_index + 1) * HEAD_DIM].astype(jnp.float32)
        value_rows = value_cache[:, :, kv_index * HEAD_DIM:(kv_index + 1) * HEAD_DIM].astype(jnp.float32)
        scores = jnp.einsum('bgd,bjd->bgj', query_heads[:, kv_index], key_rows, precision=lax.Precision.HIGHEST) * (1.0 / math.sqrt(HEAD_DIM))
        scores = jnp.where(live_mask[:, None, :], scores, masked_score)
        peak_score = lax.optimization_barrier(jnp.max(scores, axis=-1, keepdims=True))
        attn_weights = jnp.where(live_mask[:, None, :], jnp.exp(scores - peak_score), 0.0)
        denom_sum = lax.optimization_barrier(jnp.sum(attn_weights, axis=-1))
        weighted = jnp.einsum('bgj,bjd->bgd', attn_weights, value_rows, precision=lax.Precision.HIGHEST)
        outputs.append(weighted / denom_sum[..., None])
    attended = jnp.stack(outputs, axis=1).reshape(SEQS, HEADS * HEAD_DIM).astype(jnp.bfloat16)
    projected = jnp.dot(attended, out_weight, preferred_element_type=jnp.float32)
    residual = hidden_in.astype(jnp.float32) + projected
    scale_row = lax.rsqrt(lax.optimization_barrier(jnp.sum(residual * residual, axis=-1)) / D + norm_eps)
    gained = residual * norm_gain
    logits = jnp.dot(gained, router.astype(jnp.float32), precision=lax.Precision.HIGHEST) * scale_row[:, None]
    normed = (gained * scale_row[:, None]).astype(jnp.bfloat16)
    onehot_int = (expert_ids[:, :, None] == jnp.arange(EXPERTS, dtype=jnp.int32)[None, None, :]).astype(jnp.int32)
    name_count = lax.optimization_barrier(jnp.sum(onehot_int, axis=1))
    row_order = jnp.arange(SEQS, dtype=jnp.int32)
    row_block = row_order // TOK_DEV
    before = ((row_block[:, None] == row_block[None, :]) & (row_order[None, :] < row_order[:, None])).astype(jnp.int32)
    earlier = jnp.dot(before, name_count)
    slot_rank = lax.optimization_barrier(jnp.sum(onehot_int * earlier[:, None, :], axis=-1))
    slot_limit = lax.optimization_barrier(jnp.sum(onehot_int * capacity[None, None, :], axis=-1))
    kept_mask = (slot_rank < slot_limit).astype(jnp.float32)
    expert_indicator = onehot_int.astype(jnp.float32)
    chosen = lax.optimization_barrier(jnp.sum(expert_indicator * logits[:, None, :], axis=-1))
    gate_weight = jax.nn.sigmoid(chosen - chosen[:, ::-1])
    expert_output = lax.map(lambda mats: expert_rows(normed, mats[0], mats[1], mats[2]), (w_gate, w_up, w_down))
    selected_experts = jnp.einsum('hlw,whv->hlv', expert_indicator, expert_output, precision=lax.Precision.HIGHEST)
    combined = lax.optimization_barrier(jnp.sum((gate_weight * kept_mask)[:, :, None] * selected_experts, axis=1))
    return (residual + combined).astype(jnp.bfloat16)
```

```python
import functools
import math

import jax
import jax.numpy as jnp
from jax import lax
from jax.experimental import pallas as pl
from jax.experimental.pallas import tpu as pltpu
from jax.sharding import PartitionSpec as P

MESH = pl.DeviceIdType.MESH
HEAD_DIM = 128
LANES = 128
VMEM_BYTES = 67043328
masked_score = -1e30
norm_eps = 1e-05
F32 = jnp.float32
BF16 = jnp.bfloat16


def up(value, step):
    return -(-value // step) * step


def iota(shape, axis):
    return lax.broadcasted_iota(jnp.int32, shape, axis)


def div(value, by):
    return lax.div(value, jnp.full_like(value, by))


def rem(value, by):
    return lax.rem(value, jnp.full_like(value, by))


def dot(a, b):
    return jnp.dot(a, b, preferred_element_type=F32)


def dot_nt(a, b):
    return lax.dot_general(a, b, (((1,), (1,)), ((), ())), preferred_element_type=F32)


def ring_of(axis, count):
    me = lax.axis_index(axis)
    return me, [lax.rem(me + k, count) for k in range(count)], [lax.rem(me + count - k, count) for k in range(count)]


def weight_order(local):
    order = []
    for e in range(local):
        order += [("gate", e), ("up", e)]
        if e:
            order.append(("down", e - 1))
    return order + [("down", local - 1)]


def layer_kernel(
    dims, len_ref, cap_ref, ids_ref,
    hid_hbm, q_hbm, k_hbm, v_hbm, ow_hbm, gain_hbm, rt_hbm, wg_hbm, wu_hbm, wd_hbm,
    o_ref,
    hid, qv, kbuf, vbuf, ow, gain, rt, pool,
    qs, pk, sk, unpk, send1, recv1, buf2, buf3, idx, buf4, st4, xg, y, ysend, yrecv,
    in_sem, kv_sem, w_sem, ss1, rs1, ss2, rs2, ss3, rs3, ssi, rsi, ss4, rs4, sst, rst, ss5, rs5,
):
    n_seq, n_exp, seqs, toks, kvl, group, rv, rp, n_experts, slots = dims
    heads = kvl * group
    span = kbuf.shape[1]
    bp = y.shape[0]
    model = y.shape[1]
    width = model // n_seq
    local, ffl = wg_hbm.shape[0], wg_hbm.shape[2]
    n = n_seq * n_exp
    me, to_seq, from_seq = ring_of("seq", n_seq)
    my_e, to_exp, from_exp = ring_of("exp", n_exp)
    me_all = my_e * n_seq + me
    to_all = [lax.rem(me_all + k, n) for k in range(n)]
    from_all = [lax.rem(me_all + n - k, n) for k in range(n)]

    def where_is(p):
        return {"seq": lax.rem(p, n_seq), "exp": lax.div(p, n_seq)}

    barrier = pltpu.get_barrier_semaphore()
    for k in range(1, n):
        pl.semaphore_signal(barrier, inc=1, device_id=where_is(to_all[k]), device_id_type=MESH)

    q_copy = pltpu.make_async_copy(q_hbm, qv, in_sem.at[0])
    q_copy.start()
    kv_copies = []
    for b in range(seqs):
        pair = (
            pltpu.make_async_copy(k_hbm.at[b], kbuf.at[b], kv_sem.at[b, 0]),
            pltpu.make_async_copy(v_hbm.at[b], vbuf.at[b], kv_sem.at[b, 1]),
        )
        for c in pair:
            c.start()
        kv_copies.append(pair)
    small = [
        pltpu.make_async_copy(hid_hbm, hid, in_sem.at[1]),
        pltpu.make_async_copy(gain_hbm, gain.at[0], in_sem.at[2]),
        pltpu.make_async_copy(rt_hbm, rt, in_sem.at[3]),
    ]
    ow_copy = pltpu.make_async_copy(ow_hbm, ow, in_sem.at[4])
    for c in small + [ow_copy]:
        c.start()

    order = weight_order(local)

    def weight_copies(i):
        kind, e = order[i]
        s = i % slots
        if kind == "gate":
            return [pltpu.make_async_copy(wg_hbm.at[e], pool.at[s], w_sem.at[i])]
        if kind == "up":
            return [pltpu.make_async_copy(wu_hbm.at[e], pool.at[s], w_sem.at[i])]
        return [
            pltpu.make_async_copy(
                wd_hbm.at[e, :, pl.ds(j * ffl, ffl)], pool.at[s, pl.ds(j * ffl, ffl), :], w_sem.at[i])
            for j in range(model // ffl)
        ]

    def weight_wait(i):
        s = i % slots
        pltpu.make_async_copy(wg_hbm.at[0], pool.at[s], w_sem.at[i]).wait()

    for i in range(min(slots, len(order))):
        for c in weight_copies(i):
            c.start()

    pk[...] = jnp.zeros_like(pk)
    sk[...] = jnp.zeros_like(sk)
    qs[...] = jnp.zeros_like(qs)
    row = iota((heads * bp, 1), 0)
    row_b = rem(row, bp)
    want = jnp.where(row_b < seqs, row_b * heads + div(row, bp), -3)
    slot = iota((1, n_seq * rp), 1)
    slot_k = rem(slot, rp)
    have = jnp.where(slot_k < rv, div(slot, rp) * rv + slot_k, -2)
    unpk[...] = (want == have).astype(F32).astype(BF16)

    rowl = iota((bp, LANES), 0)
    lane = iota((bp, LANES), 1)
    mine = jnp.zeros((bp, LANES), F32)
    for t in range(toks):
        for k in range(2):
            mine = mine + jnp.where((rowl == my_e * toks + t) & (lane == k), ids_ref[k, t].astype(F32), 0.0)
    idx[my_e] = mine

    q_copy.wait()
    for h in range(heads):
        qs[h * bp:h * bp + seqs, :] = qv[:, h * HEAD_DIM:(h + 1) * HEAD_DIM].astype(F32)

    pl.semaphore_wait(barrier, n - 1)

    def send(src, dst, send_sem, recv_sem, device):
        c = pltpu.make_async_remote_copy(src, dst, send_sem, recv_sem, device_id=device, device_id_type=MESH)
        c.start()
        return c

    def spread(buf, sends, recvs, axis, mine_at, to):
        return [send(buf.at[mine_at], buf.at[mine_at], sends.at[k], recvs.at[k], {axis: to[k]}) for k in range(1, len(to))]

    def collect(buf, sends, recvs, axis, mine_at, to, frm):
        for k in range(1, len(to)):
            pltpu.make_async_remote_copy(
                buf.at[mine_at], buf.at[frm[k]], sends.at[k], recvs.at[k],
                device_id={axis: to[k]}, device_id_type=MESH).wait_recv()

    started = spread(idx, ssi, rsi, "exp", my_e, to_exp)

    first = me * span
    pos = iota((heads, span), 1) + first
    hrow = iota((heads, 1), 0)
    kv_of = div(hrow, group)
    diag = div(iota((heads, kvl * HEAD_DIM), 1), HEAD_DIM) == kv_of
    lane_h = iota((heads, LANES), 1)
    for b in range(seqs):
        qb = qs[pl.ds(b, heads, stride=bp), :]
        qd = jnp.where(diag, jnp.concatenate([qb] * kvl, axis=1), 0.0).astype(BF16)
        for c in kv_copies[b]:
            c.wait()
        live = pos < len_ref[b]
        s = jnp.where(live, dot_nt(qd, kbuf[b]) * (1.0 / math.sqrt(HEAD_DIM)), masked_score)
        m = jnp.max(s, axis=1, keepdims=True).astype(BF16).astype(F32)
        w = jnp.where(live, jnp.exp(s - m), 0.0)
        l = jnp.sum(w, axis=1, keepdims=True)
        wide = dot(w.astype(BF16), vbuf[b])
        acc = jnp.zeros((heads, HEAD_DIM), F32)
        for kv in range(kvl):
            acc = acc + jnp.where(kv_of == kv, wide[:, kv * HEAD_DIM:(kv + 1) * HEAD_DIM], 0.0)
        l_hi = l.astype(BF16).astype(F32)
        at = rem(hrow + b * heads, rv)
        stat = jnp.where(lane_h == at, m, jnp.where(
            lane_h == at + rp, l_hi, jnp.where(lane_h == at + 2 * rp, l - l_hi, 0.0)))
        h0 = 0
        while h0 < heads:
            p, k0 = divmod(b * heads + h0, rv)
            count = min(rv - k0, heads - h0)
            pk[p * rp + k0:p * rp + k0 + count, :] = acc[h0:h0 + count]
            sk[p * rp + k0:p * rp + k0 + count, :] = stat[h0:h0 + count]
            h0 += count
    for p in range(n_seq):
        pk[p * rp + rv:p * rp + rv + 1, :] = jnp.sum(sk[p * rp:(p + 1) * rp, :], axis=0, keepdims=True)
    for p in range(n_seq):
        send1[p] = pk[p * rp:(p + 1) * rp, :].astype(BF16)
    recv1[me] = send1[me]
    for k in range(1, n_seq):
        started.append(send(send1.at[to_seq[k]], recv1.at[me], ss1.at[k], rs1.at[k], {"seq": to_seq[k]}))
    for k in range(1, n_seq):
        pltpu.make_async_remote_copy(
            send1.at[to_seq[k]], recv1.at[from_seq[k]], ss1.at[k], rs1.at[k],
            device_id={"seq": to_seq[k]}, device_id_type=MESH).wait_recv()

    for p in range(n_seq):
        sk[p * rp:(p + 1) * rp, :] = recv1[p].astype(F32)
    stats = sk[pl.ds(rv, n_seq, stride=rp), :]
    fade = jnp.exp(stats - jnp.max(stats, axis=0, keepdims=True))
    sums = pltpu.roll(stats, LANES - rp, 1) + pltpu.roll(stats, LANES - 2 * rp, 1)
    den = jnp.sum(sums * fade, axis=0, keepdims=True)
    share = jnp.where(den > 0.0, fade / jnp.where(den > 0.0, den, 1.0), 0.0)
    same = (iota((rp, LANES), 1) == iota((rp, LANES), 0)) & (iota((rp, LANES), 0) < rv)
    att = jnp.zeros((rp, HEAD_DIM), F32)
    for p in range(n_seq):
        col = jnp.sum(jnp.where(same, share[p:p + 1, :], 0.0), axis=1, keepdims=True)
        att = att + sk[p * rp:(p + 1) * rp, :] * col
    buf2[me] = att.astype(BF16)
    started += spread(buf2, ss2, rs2, "seq", me, to_seq)
    for c in small:
        c.wait()
    ow_copy.wait()
    collect(buf2, ss2, rs2, "seq", me, to_seq, from_seq)

    rows = dot(unpk[...], jnp.concatenate([buf2[p] for p in range(n_seq)], axis=0))
    att_all = jnp.concatenate([rows[h * bp:(h + 1) * bp] for h in range(heads)], axis=1).astype(BF16)
    part = dot(att_all, ow[...])
    hidden = hid[...].astype(F32)
    rowc = iota((bp, width), 0)
    for t in range(toks):
        part = part + jnp.where(rowc == my_e * toks + t, hidden[t:t + 1, :], 0.0)
    buf3[my_e] = part
    started += spread(buf3, ss3, rs3, "exp", my_e, to_exp)
    collect(buf3, ss3, rs3, "exp", my_e, to_exp, from_exp)
    residual = functools.reduce(lambda a, b: a + b, [buf3[e] for e in range(n_exp)])
    gained = residual * gain[...]
    top = gained.astype(BF16)
    buf4[me] = top
    started += spread(buf4, ss4, rs4, "seq", me, to_seq)

    low = (gained - top.astype(F32)).astype(BF16)
    both = dot_nt(jnp.concatenate([top.astype(F32), low.astype(F32)], axis=0).astype(BF16), rt[...])
    pad = jnp.zeros((bp, LANES - n_experts), F32)
    logit = jnp.concatenate([both[:bp] + both[bp:], pad], axis=1)
    square = jnp.sum(residual * residual, axis=1, keepdims=True)
    st = jnp.where(lane == n_experts, square, logit)
    st_hi = st.astype(BF16).astype(F32)
    half = LANES // 2
    st4[me] = (st_hi + pltpu.roll(st - st_hi, half, 1)).astype(BF16)
    started += spread(st4, sst, rst, "seq", me, to_seq)
    own = []
    for t in range(toks):
        own.append(jnp.sum(jnp.where(rowc == my_e * toks + t, residual, 0.0), axis=0, keepdims=True))
    collect(idx, ssi, rsi, "exp", my_e, to_exp, from_exp)
    idv = functools.reduce(lambda a, b: a + b, [idx[e] for e in range(n_exp)]).astype(jnp.int32)
    ids = [idv[:, k:k + 1] for k in range(2)]
    rowb = iota((bp, 1), 0)
    place = rem(rowb, toks)
    keep = []
    for k in range(2):
        rank = jnp.zeros((bp, 1), jnp.int32)
        for d in range(1, toks):
            for j in range(2):
                before = pltpu.roll(idv, d, 0)[:, j:j + 1]
                rank = rank + jnp.where((place >= d) & (ids[k] == before), 1, 0)
        limit = jnp.zeros((bp, 1), jnp.int32)
        for e in range(n_experts):
            limit = limit + jnp.where(ids[k] == e, cap_ref[e], 0)
        keep.append((rank < limit) & (rowb < seqs))

    collect(buf4, ss4, rs4, "seq", me, to_seq, from_seq)
    for p in range(n_seq):
        xg[:, p * width:(p + 1) * width] = buf4[p]
    x = xg[...]

    def product(i):
        weight_wait(i)
        return dot(x, pool[i % slots])

    def refill(i):
        if i + slots < len(order):
            for c in weight_copies(i + slots):
                c.start()

    scale = None
    coef = None
    gates = {}
    hidden_of = {}
    for i, (kind, e) in enumerate(order):
        if kind == "gate":
            gates[e] = product(i)
        elif kind == "up":
            u = product(i)
            if scale is None:
                collect(st4, sst, rst, "seq", me, to_seq, from_seq)
                tot = functools.reduce(lambda a, b: a + b, [st4[p].astype(F32) for p in range(n_seq)])
                tot = tot + pltpu.roll(tot, half, 1)
                scale = lax.rsqrt(tot[:, n_experts:n_experts + 1] / model + norm_eps)
                logits = jnp.where(lane < n_experts, tot, 0.0) * scale
                chosen = [jnp.sum(jnp.where(lane == ids[k], logits, 0.0), axis=1, keepdims=True) for k in range(2)]
                coef = [jnp.where(keep[k], jax.nn.sigmoid(chosen[k] - chosen[1 - k]), 0.0) for k in range(2)]
            ge = my_e * local + e
            c = jnp.where(ids[0] == ge, coef[0], 0.0) + jnp.where(ids[1] == ge, coef[1], 0.0)
            hidden_of[e] = (jax.nn.silu(gates[e] * scale) * (u * scale) * c).astype(BF16)
        else:
            weight_wait(i)
            for j in range(model // ffl):
                cols = slice(j * ffl, (j + 1) * ffl)
                part = dot(hidden_of[e], pool[i % slots, cols, :])
                y[:, cols] = part if e == 0 else y[:, cols] + part
        refill(i)

    for e in range(n_exp):
        rows = y[e * toks:(e + 1) * toks, :].astype(BF16)
        for s in range(n_seq):
            ysend[e * n_seq + s] = rows[:, s * width:(s + 1) * width]
    yrecv[me_all] = ysend[me_all]
    for k in range(1, n):
        started.append(send(ysend.at[to_all[k]], yrecv.at[me_all], ss5.at[k], rs5.at[k], where_is(to_all[k])))
    total = jnp.concatenate(own, axis=0)
    for k in range(1, n):
        pltpu.make_async_remote_copy(
            ysend.at[to_all[k]], yrecv.at[from_all[k]], ss5.at[k], rs5.at[k],
            device_id=where_is(to_all[k]), device_id_type=MESH).wait_recv()
    for p in range(n):
        total = total + yrecv[p].astype(F32)
    o_ref[...] = total.astype(BF16)
    for c in started:
        c.wait_send()


def on_device(
    n_seq, n_exp, hidden_in, queries, key_cache, value_cache, lengths, out_weight, norm_gain,
    router, expert_ids, capacity, w_gate, w_up, w_down,
):
    seqs = queries.shape[0]
    toks, width = hidden_in.shape
    span, kv_width = key_cache.shape[1:]
    kvl = kv_width // HEAD_DIM
    heads = queries.shape[1] // HEAD_DIM
    group = heads // kvl
    bp = up(seqs, 8)
    n_experts = router.shape[1]
    model = width * n_seq
    local, _, ffl = w_gate.shape
    rv = -(-seqs * heads // n_seq)
    rp = up(rv + 1, 16)
    n = n_seq * n_exp
    fixed = 2 * (2 * seqs * span * kv_width + out_weight.size)
    spare = 7 << 18
    slots = min(3 * local, (VMEM_BYTES - fixed - spare) // (2 * model * ffl))
    vmem = pl.BlockSpec(memory_space=pltpu.VMEM)
    smem = pl.BlockSpec(memory_space=pltpu.SMEM)
    hbm = pl.BlockSpec(memory_space=pltpu.HBM)
    dma = pltpu.SemaphoreType.DMA
    return pl.pallas_call(
        functools.partial(layer_kernel, (n_seq, n_exp, seqs, toks, kvl, group, rv, rp, n_experts, slots)),
        in_specs=[smem, smem, smem] + [hbm] * 10,
        out_specs=vmem,
        out_shape=jax.ShapeDtypeStruct((toks, width), BF16),
        scratch_shapes=[
            pltpu.VMEM((toks, width), BF16),
            pltpu.VMEM(queries.shape, BF16),
            pltpu.VMEM(key_cache.shape, BF16),
            pltpu.VMEM(value_cache.shape, BF16),
            pltpu.VMEM(out_weight.shape, BF16),
            pltpu.VMEM((1, width), F32),
            pltpu.VMEM((n_experts, width), BF16),
            pltpu.VMEM((slots, model, ffl), BF16),
            pltpu.VMEM((heads * bp, HEAD_DIM), F32),
            pltpu.VMEM((n_seq * rp, HEAD_DIM), F32),
            pltpu.VMEM((n_seq * rp, HEAD_DIM), F32),
            pltpu.VMEM((heads * bp, n_seq * rp), BF16),
            pltpu.VMEM((n_seq, rp, HEAD_DIM), BF16),
            pltpu.VMEM((n_seq, rp, HEAD_DIM), BF16),
            pltpu.VMEM((n_seq, rp, HEAD_DIM), BF16),
            pltpu.VMEM((n_exp, bp, width), F32),
            pltpu.VMEM((n_exp, bp, LANES), F32),
            pltpu.VMEM((n_seq, bp, width), BF16),
            pltpu.VMEM((n_seq, bp, LANES), BF16),
            pltpu.VMEM((bp, model), BF16),
            pltpu.VMEM((bp, model), F32),
            pltpu.VMEM((n, toks, width), BF16),
            pltpu.VMEM((n, toks, width), BF16),
            dma((5,)), dma((seqs, 2)), dma((3 * local,)),
            dma((n_seq,)), dma((n_seq,)), dma((n_seq,)), dma((n_seq,)),
            dma((n_exp,)), dma((n_exp,)), dma((n_exp,)), dma((n_exp,)),
            dma((n_seq,)), dma((n_seq,)), dma((n_seq,)), dma((n_seq,)),
            dma((n,)), dma((n,)),
        ],
        compiler_params=pltpu.CompilerParams(
            collective_id=0, has_side_effects=True, vmem_limit_bytes=VMEM_BYTES),
        name="layer",
    )(
        lengths, capacity, expert_ids.T, hidden_in, queries, key_cache, value_cache, out_weight, norm_gain,
        router.T, w_gate, w_up, w_down,
    )


def solution(mesh):
    in_specs = (
        P("exp", "seq"),
        P(None, "exp"),
        P(None, "seq", "exp"),
        P(None, "seq", "exp"),
        P(),
        P("exp", "seq"),
        P("seq"),
        P("seq", None),
        P("exp", None),
        P(),
        P("exp", None, "seq"),
        P("exp", None, "seq"),
        P("exp", "seq", None),
    )
    return jax.shard_map(
        functools.partial(on_device, mesh.shape["seq"], mesh.shape["exp"]),
        mesh=mesh, in_specs=in_specs, out_specs=P("exp", "seq"), check_vma=False,
    )
```

```python
import functools
import math

import jax
import jax.numpy as jnp
from jax import lax
from jax.experimental import pallas as pl
from jax.experimental.pallas import tpu as pltpu
from jax.sharding import PartitionSpec as P

MESH = pl.DeviceIdType.MESH
HEAD_DIM = 128
LANES = 128
VMEM_BYTES = 67043328
PRIORITY = 1
BATCH = 3
masked_score = -1e30
norm_eps = 1e-05
F32 = jnp.float32
BF16 = jnp.bfloat16


def up(value, step):
    return -(-value // step) * step


def iota(shape, axis):
    return lax.broadcasted_iota(jnp.int32, shape, axis)


def div(value, by):
    return lax.div(value, jnp.full_like(value, by))


def rem(value, by):
    return lax.rem(value, jnp.full_like(value, by))


def dot(a, b):
    return jnp.dot(a, b, preferred_element_type=F32)


def dot_nt(a, b):
    return lax.dot_general(a, b, (((1,), (1,)), ((), ())), preferred_element_type=F32)


def partner(at, step, count):
    if count & (count - 1):
        return lax.rem(at + step, count)
    bit = 1
    out = at
    while bit < count:
        if step & bit:
            out = out + bit * (1 - 2 * lax.rem(lax.div(at, bit), 2))
        bit *= 2
    return out


def ring_of(axis, count):
    me = lax.axis_index(axis)
    return me, [partner(me, k, count) for k in range(count)]


def layer_kernel(
    dims, len_hbm, cap_hbm, ids_hbm, hid_hbm, q_hbm, k_hbm, v_hbm, ow_hbm, gain_hbm, rt_hbm, wg_hbm, wu_hbm, wd_hbm,
    o_ref,
    len_ref, cap_ref, ids_ref, hid, qv, kbuf, vbuf, ow, gain, rt, pool,
    qs, pk, sk, unpk, send1, recv1, buf2, buf3, idx, buf4, st4, gu, ysend, yrecv,
    in_sem, kv_sem, w_sem, sem1, sem2, sem3, semi, sem4, sems, sem5,
):
    n_seq, n_exp, seqs, toks, kvl, group, rv, rp, n_experts, slots = dims
    heads = kvl * group
    span = kbuf.shape[1]
    bp = gu.shape[1]
    model, ffl = pool.shape[1:]
    width = model // n_seq
    local = wg_hbm.shape[0]
    n = n_seq * n_exp
    chunks = 2 * local
    kc = model // chunks
    in_chunk = n_seq // chunks
    cols = model // local
    in_block = n_seq // local
    me, to_seq = ring_of("seq", n_seq)
    my_e, to_exp = ring_of("exp", n_exp)
    me_all = my_e * n_seq + me
    to_all = [lax.rem(me_all + k, n) for k in range(n)]
    my_chunk, chunk_pos = lax.div(me, in_chunk), lax.rem(me, in_chunk)
    my_block, block_pos = lax.div(me, in_block), lax.rem(me, in_block)
    chunk_at = [partner(my_chunk, i, chunks) for i in range(chunks)]
    block_at = [partner(my_block, local - 1 - i, local) for i in range(local)]

    def chunk_members(i):
        return [
            (to_exp[k], chunk_at[i] * in_chunk + lax.rem(chunk_pos + r, in_chunk))
            for r in range(in_chunk) for k in range(n_exp)
        ]

    def where_is(p):
        return {"seq": lax.rem(p, n_seq), "exp": lax.div(p, n_seq)}

    q_copy = pltpu.make_async_copy(q_hbm, qv, in_sem.at[0])
    q_copy.start()
    numbers = [
        pltpu.make_async_copy(len_hbm, len_ref, in_sem.at[5]),
        pltpu.make_async_copy(cap_hbm, cap_ref, in_sem.at[6]),
        pltpu.make_async_copy(ids_hbm, ids_ref, in_sem.at[7]),
    ]
    for c in numbers:
        c.start()
    for b in range(seqs):
        pair = (
            pltpu.make_async_copy(k_hbm.at[b], kbuf.at[b], kv_sem.at[b // BATCH, 0]),
            pltpu.make_async_copy(v_hbm.at[b], vbuf.at[b], kv_sem.at[b // BATCH, 1]),
        )
        for c in pair:
            c.start(priority=0 if b < BATCH else 1)
    small = [
        pltpu.make_async_copy(hid_hbm, hid, in_sem.at[1]),
        pltpu.make_async_copy(gain_hbm, gain.at[0], in_sem.at[2]),
        pltpu.make_async_copy(rt_hbm, rt, in_sem.at[3]),
    ]
    ow_copy = pltpu.make_async_copy(ow_hbm, ow, in_sem.at[4])
    barrier = pltpu.get_barrier_semaphore()
    for k in range(1, n):
        pl.semaphore_signal(barrier, inc=1, device_id=where_is(to_all[k]), device_id_type=MESH)


    def weight_start(i):
        s = i % slots
        if i < chunks:
            rows = pl.ds(pl.multiple_of(chunk_at[i] * kc, kc), kc)
            for e in range(local):
                for half, w in enumerate((wg_hbm, wu_hbm)):
                    at = (2 * e + half) * kc
                    pltpu.make_async_copy(w.at[e, rows, :], pool.at[s, pl.ds(at, kc), :], w_sem.at[i]).start(priority=PRIORITY)
        else:
            for j in range(cols // ffl):
                part = pl.ds(pl.multiple_of(block_at[i - chunks] * cols + j * ffl, ffl), ffl)
                for e in range(local):
                    at = (j * local + e) * ffl
                    pltpu.make_async_copy(wd_hbm.at[e, :, part], pool.at[s, pl.ds(at, ffl), :], w_sem.at[i]).start(priority=PRIORITY)

    def weight_wait(i):
        pltpu.make_async_copy(wg_hbm.at[0], pool.at[i % slots], w_sem.at[i]).wait()

    loads = chunks + local

    def refill(i):
        if i + slots < loads:
            weight_start(i + slots)

    ahead = min(slots, loads)
    turn = min(5, ahead)
    waves = [range(turn), range(turn, ahead)]

    pk[...] = jnp.zeros_like(pk)
    sk[...] = jnp.zeros_like(sk)
    qs[...] = jnp.zeros_like(qs)
    row = iota((heads * bp, 1), 0)
    row_b = rem(row, bp)
    want = jnp.where(row_b < seqs, row_b * heads + div(row, bp), -3)
    slot = iota((1, n_seq * rp), 1)
    slot_k = rem(slot, rp)
    have = jnp.where(slot_k < rv, div(slot, rp) * rv + slot_k, -2)
    unpk[...] = (want == have).astype(F32).astype(BF16)

    q_copy.wait()
    for h in range(heads):
        qs[h * bp:h * bp + seqs, :] = qv[:, h * HEAD_DIM:(h + 1) * HEAD_DIM].astype(F32)

    rowl = iota((bp, LANES), 0)
    lane = iota((bp, LANES), 1)
    for c in numbers:
        c.wait()
    mine = jnp.zeros((bp, LANES), F32)
    for t in range(toks):
        for k in range(2):
            mine = mine + jnp.where((rowl == my_e * toks + t) & (lane == k), ids_ref[k, t].astype(F32), 0.0)
    idx[my_e] = mine

    def send(src, dst, send_sem, recv_sem, device):
        c = pltpu.make_async_remote_copy(src, dst, send_sem, recv_sem, device_id=device, device_id_type=MESH)
        c.start()
        return c

    peer = {"seq": to_seq[1 % n_seq], "exp": to_exp[1 % n_exp]}

    def whole(buf, count, sems):
        part = buf.at[pl.ds(0, count)]
        return pltpu.make_async_remote_copy(part, part, sems.at[0], sems.at[1], device_id=peer, device_id_type=MESH)

    def spread(buf, sems, axis, mine_at, to):
        for k in reversed(range(1, len(to))):
            send(buf.at[mine_at], buf.at[mine_at], sems.at[0], sems.at[1], {axis: to[k]})
        return whole(buf, len(to) - 1, sems)

    first = me * span
    pos = iota((heads, span), 1) + first
    hrow = iota((heads, 1), 0)
    kv_of = div(hrow, group)
    diag = div(iota((heads, kvl * HEAD_DIM), 1), HEAD_DIM) == kv_of
    lane_h = iota((heads, LANES), 1)

    def attend(batch):
        scores = []
        for b in batch:
            qb = qs[pl.ds(b, heads, stride=bp), :]
            qd = jnp.where(diag, jnp.concatenate([qb] * kvl, axis=1), 0.0).astype(BF16)
            scores.append(dot_nt(qd, kbuf[b]) * (1.0 / math.sqrt(HEAD_DIM)))
        weights = []
        for b, s in zip(batch, scores):
            live = pos < len_ref[b]
            m = jnp.max(jnp.where(live, s, masked_score), axis=1, keepdims=True).astype(BF16).astype(F32)
            w = jnp.where(live, jnp.exp(s - m), 0.0)
            weights.append((m, jnp.sum(w, axis=1, keepdims=True), w.astype(BF16)))
        for b, (m, l, w) in zip(batch, weights):
            wide = dot(w, vbuf[b])
            acc = jnp.zeros((heads, HEAD_DIM), F32)
            for kv in range(kvl):
                acc = acc + jnp.where(kv_of == kv, wide[:, kv * HEAD_DIM:(kv + 1) * HEAD_DIM], 0.0)
            l_hi = l.astype(BF16).astype(F32)
            at = rem(hrow + b * heads, rv)
            stat = jnp.where(lane_h == at, m, jnp.where(
                lane_h == at + rp, l_hi, jnp.where(lane_h == at + 2 * rp, l - l_hi, 0.0)))
            h0 = 0
            while h0 < heads:
                p, k0 = divmod(b * heads + h0, rv)
                count = min(rv - k0, heads - h0)
                pk[p * rp + k0:p * rp + k0 + count, :] = acc[h0:h0 + count]
                sk[p * rp + k0:p * rp + k0 + count, :] = stat[h0:h0 + count]
                h0 += count

    per = BATCH
    for b0 in range(0, seqs, per):
        batch = range(b0, min(b0 + per, seqs))
        some = pl.ds(b0, len(batch))
        pltpu.make_async_copy(k_hbm.at[some], kbuf.at[some], kv_sem.at[b0 // BATCH, 0]).wait()
        pltpu.make_async_copy(v_hbm.at[some], vbuf.at[some], kv_sem.at[b0 // BATCH, 1]).wait()
        if b0 + per >= seqs:
            for c in small + [ow_copy]:
                c.start()
            for i in waves[0]:
                weight_start(i)
        attend(batch)
    for p in range(n_seq):
        pk[p * rp + rv:p * rp + rv + 1, :] = jnp.sum(sk[p * rp:(p + 1) * rp, :], axis=0, keepdims=True)
    for p in range(n_seq):
        send1[p] = pk[p * rp:(p + 1) * rp, :].astype(BF16)
    recv1[me] = send1[me]
    pl.semaphore_wait(barrier, n - 1)
    for k in reversed(range(1, n_seq)):
        send(send1.at[to_seq[k]], recv1.at[me], sem1.at[0], sem1.at[1], {"seq": to_seq[k]})
    out1 = whole(recv1, n_seq - 1, sem1)
    outi = spread(idx, semi, "exp", my_e, to_exp)
    out1.wait_recv()
    for i in waves[1]:
        weight_start(i)
    for p in range(n_seq):
        sk[p * rp:(p + 1) * rp, :] = recv1[p].astype(F32)
    stats = sk[pl.ds(rv, n_seq, stride=rp), :]
    fade = jnp.exp(stats - jnp.max(stats, axis=0, keepdims=True))
    sums = pltpu.roll(stats, LANES - rp, 1) + pltpu.roll(stats, LANES - 2 * rp, 1)
    den = jnp.sum(sums * fade, axis=0, keepdims=True)
    share = jnp.where(den > 0.0, fade / jnp.where(den > 0.0, den, 1.0), 0.0)
    same = (iota((rp, LANES), 1) == iota((rp, LANES), 0)) & (iota((rp, LANES), 0) < rv)
    att = jnp.zeros((rp, HEAD_DIM), F32)
    for p in range(n_seq):
        col = jnp.sum(jnp.where(same, share[p:p + 1, :], 0.0), axis=1, keepdims=True)
        att = att + sk[p * rp:(p + 1) * rp, :] * col
    buf2[me] = att.astype(BF16)
    out2 = spread(buf2, sem2, "seq", me, to_seq)
    for c in small:
        c.wait()
    ow_copy.wait()
    outi.wait_recv()
    idv = functools.reduce(lambda a, b: a + b, [idx[e] for e in range(n_exp)]).astype(jnp.int32)
    ids = [idv[:, k:k + 1] for k in range(2)]
    rowb = iota((bp, 1), 0)
    place = rem(rowb, toks)
    keep = []
    for k in range(2):
        rank = jnp.zeros((bp, 1), jnp.int32)
        for d in range(1, toks):
            for j in range(2):
                before = pltpu.roll(idv, d, 0)[:, j:j + 1]
                rank = rank + jnp.where((place >= d) & (ids[k] == before), 1, 0)
        limit = jnp.zeros((bp, 1), jnp.int32)
        for e in range(n_experts):
            limit = limit + jnp.where(ids[k] == e, cap_ref[e], 0)
        keep.append((rank < limit) & (rowb < seqs))
    out2.wait_recv()

    rows = dot(unpk[...], jnp.concatenate([buf2[p] for p in range(n_seq)], axis=0))
    att_all = jnp.concatenate([rows[h * bp:(h + 1) * bp] for h in range(heads)], axis=1).astype(BF16)
    part = dot(att_all, ow[...])
    hidden = hid[...].astype(F32)
    rowc = iota((bp, width), 0)
    for t in range(toks):
        part = part + jnp.where(rowc == my_e * toks + t, hidden[t:t + 1, :], 0.0)
    here = me * n_exp + my_e
    buf4[here] = (part * gain[...]).astype(BF16)
    buf3[my_e] = part
    group_size = in_chunk * n_exp
    both_ways = chunks & (chunks - 1) == 0
    for i in range(chunks):
        for at, (to_e, to_s) in enumerate(chunk_members(i)):
            if i or at:
                back = (in_chunk - at // n_exp) % in_chunk * n_exp + (n_exp - at % n_exp) % n_exp
                arrival = group_size + (i if both_ways else chunks - i) if i else back
                send(buf4.at[here], buf4.at[here], sem4.at[0], sem4.at[arrival], {"seq": to_s, "exp": to_e})
        if i == 0:
            out3 = spread(buf3, sem3, "exp", my_e, to_exp)
    out4 = pltpu.make_async_remote_copy(
        buf4.at[pl.ds(0, n - 1)], buf4.at[pl.ds(0, n - 1)], sem4.at[0], sem4.at[1], device_id=peer, device_id_type=MESH)

    half = LANES // 2

    for i in range(chunks):
        if i:
            part = buf4.at[pl.ds(chunk_at[i] * group_size, group_size)]
            pltpu.make_async_remote_copy(
                part, part, sem4.at[0], sem4.at[group_size + i], device_id=peer, device_id_type=MESH).wait_recv()
        else:
            for at, (of_e, of_s) in enumerate(chunk_members(0)):
                if at:
                    part = buf4.at[of_s * n_exp + of_e]
                    pltpu.make_async_remote_copy(
                        part, part, sem4.at[0], sem4.at[at], device_id=peer, device_id_type=MESH).wait_recv()
        if i == chunks - 1:
            outs.wait_recv()
            tot = functools.reduce(lambda a, b: a + b, [st4[p].astype(F32) for p in range(n_seq)])
            tot = tot + pltpu.roll(tot, half, 1)
            scale = lax.rsqrt(tot[:, n_experts:n_experts + 1] / model + norm_eps)
            logits = jnp.where(lane < n_experts, tot, 0.0) * scale
            chosen = [jnp.sum(jnp.where(lane == ids[k], logits, 0.0), axis=1, keepdims=True) for k in range(2)]
            coef = [jnp.where(keep[k], jax.nn.sigmoid(chosen[k] - chosen[1 - k]), 0.0) for k in range(2)]
        if i == 0:
            out3.wait_recv()
        weight_wait(i)
        s = i % slots
        if i == 0:
            residual = functools.reduce(lambda a, b: a + b, [buf3[e] for e in range(n_exp)])
            gained = residual * gain[...]
            top = gained.astype(BF16).astype(F32)
            both = dot_nt(jnp.concatenate([top, gained - top], axis=0).astype(BF16), rt[...])
            pad = jnp.zeros((bp, LANES - n_experts), F32)
            logit = jnp.concatenate([both[:bp] + both[bp:], pad], axis=1)
            square = jnp.sum(residual * residual, axis=1, keepdims=True)
            st = jnp.where(lane == n_experts, square, logit)
            st_hi = st.astype(BF16).astype(F32)
            st4[me] = (st_hi + pltpu.roll(st - st_hi, half, 1)).astype(BF16)
            own = jnp.concatenate([
                jnp.sum(jnp.where(rowc == my_e * toks + t, residual, 0.0), axis=0, keepdims=True) for t in range(toks)
            ], axis=0)
        pieces = []
        for r in range(in_chunk):
            at = chunk_at[i] * in_chunk + r
            pieces.append(functools.reduce(lambda a, b: a + b, [buf4[at * n_exp + e].astype(F32) for e in range(n_exp)]))
        x = jnp.concatenate(pieces, axis=1).astype(BF16)
        for m in range(chunks):
            part = dot(x, pool[s, m * kc:(m + 1) * kc, :])
            gu[m] = part if i == 0 else gu[m] + part
        refill(i)
        if i == 0:
            outs = spread(st4, sems, "seq", me, to_seq)

    inner = []
    for e in range(local):
        ge = my_e * local + e
        c = jnp.where(ids[0] == ge, coef[0], 0.0) + jnp.where(ids[1] == ge, coef[1], 0.0)
        inner.append(jax.nn.silu(gu[2 * e] * scale) * (gu[2 * e + 1] * scale) * c)
    inner = jnp.concatenate(inner, axis=1).astype(BF16)

    for i in range(local):
        weight_wait(chunks + i)
        s = (chunks + i) % slots
        deep = local * ffl
        y = jnp.concatenate(
            [dot(inner, pool[s, j * deep:(j + 1) * deep, :]) for j in range(cols // ffl)], axis=1).astype(BF16)
        base = block_at[i] * in_block
        for e in range(n_exp):
            for r in range(in_block):
                ysend[e * n_seq + base + r] = y[e * toks:(e + 1) * toks, r * width:(r + 1) * width]
        refill(chunks + i)
        for r in range(in_block):
            for k in range(n_exp):
                to_s = base + lax.rem(block_pos + r, in_block)
                to = to_exp[k] * n_seq + to_s
                if i == local - 1 and r == 0 and k == 0:
                    yrecv[me_all] = ysend[me_all]
                else:
                    send(ysend.at[to], yrecv.at[me_all], sem5.at[0], sem5.at[1], {"seq": to_s, "exp": to_exp[k]})
    out5 = whole(yrecv, n - 1, sem5)
    for c in (out1, outi, out2, out3, out4, outs):
        c.wait_send()
    total = own
    out5.wait_recv()
    for p in range(n):
        total = total + yrecv[p].astype(F32)
    o_ref[...] = total.astype(BF16)
    out5.wait_send()


def on_device(
    n_seq, n_exp, hidden_in, queries, key_cache, value_cache, lengths, out_weight, norm_gain,
    router, expert_ids, capacity, w_gate, w_up, w_down,
):
    seqs = queries.shape[0]
    toks, width = hidden_in.shape
    span, kv_width = key_cache.shape[1:]
    kvl = kv_width // HEAD_DIM
    heads = queries.shape[1] // HEAD_DIM
    group = heads // kvl
    bp = up(seqs, 8)
    n_experts = router.shape[1]
    model = width * n_seq
    local, _, ffl = w_gate.shape
    rv = -(-seqs * heads // n_seq)
    rp = up(rv + 1, 16)
    n = n_seq * n_exp
    fixed = 2 * (2 * seqs * span * kv_width + out_weight.size)
    spare = 7 << 18
    slots = min(3 * local, (VMEM_BYTES - fixed - spare) // (2 * model * ffl))
    vmem = pl.BlockSpec(memory_space=pltpu.VMEM)
    hbm = pl.BlockSpec(memory_space=pltpu.HBM)
    dma = pltpu.SemaphoreType.DMA
    return pl.pallas_call(
        functools.partial(layer_kernel, (n_seq, n_exp, seqs, toks, kvl, group, rv, rp, n_experts, slots)),
        in_specs=[hbm] * 13,
        out_specs=vmem,
        out_shape=jax.ShapeDtypeStruct((toks, width), BF16),
        scratch_shapes=[
            pltpu.SMEM(lengths.shape, jnp.int32),
            pltpu.SMEM(capacity.shape, jnp.int32),
            pltpu.SMEM(expert_ids.shape[::-1], jnp.int32),
            pltpu.VMEM((toks, width), BF16),
            pltpu.VMEM(queries.shape, BF16),
            pltpu.VMEM(key_cache.shape, BF16),
            pltpu.VMEM(value_cache.shape, BF16),
            pltpu.VMEM(out_weight.shape, BF16),
            pltpu.VMEM((1, width), F32),
            pltpu.VMEM((n_experts, width), BF16),
            pltpu.VMEM((slots, model, ffl), BF16),
            pltpu.VMEM((heads * bp, HEAD_DIM), F32),
            pltpu.VMEM((n_seq * rp, HEAD_DIM), F32),
            pltpu.VMEM((n_seq * rp, HEAD_DIM), F32),
            pltpu.VMEM((heads * bp, n_seq * rp), BF16),
            pltpu.VMEM((n_seq, rp, HEAD_DIM), BF16),
            pltpu.VMEM((n_seq, rp, HEAD_DIM), BF16),
            pltpu.VMEM((n_seq, rp, HEAD_DIM), BF16),
            pltpu.VMEM((n_exp, bp, width), F32),
            pltpu.VMEM((n_exp, bp, LANES), F32),
            pltpu.VMEM((n, bp, width), BF16),
            pltpu.VMEM((n_seq, bp, LANES), BF16),
            pltpu.VMEM((2 * local, bp, ffl), F32),
            pltpu.VMEM((n, toks, width), BF16),
            pltpu.VMEM((n, toks, width), BF16),
            dma((8,)), dma((-(-seqs // BATCH), 2)), dma((3 * local,)),
            dma((2,)), dma((2,)), dma((2,)), dma((2,)), dma((n // (2 * local) + 2 * local,)), dma((2,)), dma((2,)),
        ],
        compiler_params=pltpu.CompilerParams(
            collective_id=0, has_side_effects=True, vmem_limit_bytes=VMEM_BYTES),
        name="layer",
    )(
        lengths, capacity, expert_ids.T, hidden_in, queries, key_cache, value_cache, out_weight, norm_gain,
        router.T, w_gate, w_up, w_down,
    )


def solution(mesh):
    in_specs = (
        P("exp", "seq"),
        P(None, "exp"),
        P(None, "seq", "exp"),
        P(None, "seq", "exp"),
        P(),
        P("exp", "seq"),
        P("seq"),
        P("seq", None),
        P("exp", None),
        P(),
        P("exp", None, "seq"),
        P("exp", None, "seq"),
        P("exp", "seq", None),
    )
    return jax.shard_map(
        functools.partial(on_device, mesh.shape["seq"], mesh.shape["exp"]),
        mesh=mesh, in_specs=in_specs, out_specs=P("exp", "seq"), check_vma=False,
    )
```

```python
import functools
import math

import jax
import jax.numpy as jnp
from jax import lax
from jax.experimental import pallas as pl
from jax.experimental.pallas import tpu as pltpu
from jax.sharding import PartitionSpec as P

MESH = pl.DeviceIdType.MESH
HEAD_DIM = 128
LANES = 128
VMEM_BYTES = 67043328 - (1 << 19)
PRIORITY = 1
BATCH = 3
masked_score = -1e30
norm_eps = 1e-05
F32 = jnp.float32
BF16 = jnp.bfloat16


def up(value, step):
    return -(-value // step) * step


def iota(shape, axis):
    return lax.broadcasted_iota(jnp.int32, shape, axis)


def div(value, by):
    return lax.div(value, jnp.full_like(value, by))


def rem(value, by):
    return lax.rem(value, jnp.full_like(value, by))


def dot(a, b):
    return jnp.dot(a, b, preferred_element_type=F32)


def dot_nt(a, b):
    return lax.dot_general(a, b, (((1,), (1,)), ((), ())), preferred_element_type=F32)


def partner(at, step, count):
    if count & (count - 1):
        return lax.rem(at + step, count)
    bit = 1
    out = at
    while bit < count:
        if step & bit:
            out = out + bit * (1 - 2 * lax.rem(lax.div(at, bit), 2))
        bit *= 2
    return out


def ring_of(axis, count):
    me = lax.axis_index(axis)
    return me, [partner(me, k, count) for k in range(count)]


def layer_kernel(
    dims, len_hbm, cap_hbm, ids_hbm, hid_hbm, q_hbm, k_hbm, v_hbm, ow_hbm, gain_hbm, rt_hbm, wg_hbm, wu_hbm, wd_hbm,
    o_ref,
    len_ref, cap_ref, ids_ref, hid, qv, kbuf, vbuf, ow, gain, rt, pool,
    qs, pk, sk, unpk, send1, recv1, buf2, buf3, idx, buf4, st4, gu, ysend, yrecv,
    in_sem, kv_sem, w_sem, sem1, sem2, sem3, semi, sem4, sems, sem5,
):
    n_seq, n_exp, seqs, toks, kvl, group, rv, rp, n_experts, slots = dims
    heads = kvl * group
    span = kbuf.shape[1]
    bp = gu.shape[1]
    model, ffl = pool.shape[1:]
    width = model // n_seq
    local = wg_hbm.shape[0]
    n = n_seq * n_exp
    chunks = 2 * local
    kc = model // chunks
    in_chunk = n_seq // chunks
    cols = model // local
    in_block = n_seq // local
    me, to_seq = ring_of("seq", n_seq)
    my_e, to_exp = ring_of("exp", n_exp)
    me_all = my_e * n_seq + me
    to_all = [lax.rem(me_all + k, n) for k in range(n)]
    my_chunk, chunk_pos = lax.div(me, in_chunk), lax.rem(me, in_chunk)
    my_block, block_pos = lax.div(me, in_block), lax.rem(me, in_block)
    chunk_at = [partner(my_chunk, i, chunks) for i in range(chunks)]
    block_at = [partner(my_block, local - 1 - i, local) for i in range(local)]

    def chunk_members(i):
        return [
            (to_exp[k], chunk_at[i] * in_chunk + lax.rem(chunk_pos + r, in_chunk))
            for r in range(in_chunk) for k in range(n_exp)
        ]

    def where_is(p):
        return {"seq": lax.rem(p, n_seq), "exp": lax.div(p, n_seq)}

    q_copy = pltpu.make_async_copy(q_hbm, qv, in_sem.at[0])
    q_copy.start()
    numbers = [
        pltpu.make_async_copy(len_hbm, len_ref, in_sem.at[5]),
        pltpu.make_async_copy(cap_hbm, cap_ref, in_sem.at[6]),
        pltpu.make_async_copy(ids_hbm, ids_ref, in_sem.at[7]),
    ]
    for c in numbers:
        c.start()
    for b in range(seqs):
        pair = (
            pltpu.make_async_copy(k_hbm.at[b], kbuf.at[b], kv_sem.at[b // BATCH, 0]),
            pltpu.make_async_copy(v_hbm.at[b], vbuf.at[b], kv_sem.at[b // BATCH, 1]),
        )
        for c in pair:
            c.start(priority=0 if b < BATCH else 1)
    small = [
        pltpu.make_async_copy(hid_hbm, hid, in_sem.at[1]),
        pltpu.make_async_copy(gain_hbm, gain.at[0], in_sem.at[2]),
        pltpu.make_async_copy(rt_hbm, rt, in_sem.at[3]),
    ]
    ow_copy = pltpu.make_async_copy(ow_hbm, ow, in_sem.at[4])
    barrier = pltpu.get_barrier_semaphore()
    for k in range(1, n):
        pl.semaphore_signal(barrier, inc=1, device_id=where_is(to_all[k]), device_id_type=MESH)


    def weight_start(i):
        s = i % slots
        if i < chunks:
            rows = pl.ds(pl.multiple_of(chunk_at[i] * kc, kc), kc)
            for e in range(local):
                for half, w in enumerate((wg_hbm, wu_hbm)):
                    at = (2 * e + half) * kc
                    pltpu.make_async_copy(w.at[e, rows, :], pool.at[s, pl.ds(at, kc), :], w_sem.at[i]).start(priority=PRIORITY)
        else:
            for j in range(cols // ffl):
                part = pl.ds(pl.multiple_of(block_at[i - chunks] * cols + j * ffl, ffl), ffl)
                for e in range(local):
                    at = (j * local + e) * ffl
                    pltpu.make_async_copy(wd_hbm.at[e, :, part], pool.at[s, pl.ds(at, ffl), :], w_sem.at[i]).start(priority=PRIORITY)

    def weight_wait(i):
        pltpu.make_async_copy(wg_hbm.at[0], pool.at[i % slots], w_sem.at[i]).wait()

    loads = chunks + local

    def refill(i):
        if i + slots < loads:
            weight_start(i + slots)

    ahead = min(slots, loads)
    turn = min(5, ahead)
    waves = [range(turn), range(turn, ahead)]

    pk[...] = jnp.zeros_like(pk)
    sk[...] = jnp.zeros_like(sk)
    qs[...] = jnp.zeros_like(qs)
    row = iota((heads * bp, 1), 0)
    row_b = rem(row, bp)
    want = jnp.where(row_b < seqs, row_b * heads + div(row, bp), -3)
    slot = iota((1, n_seq * rp), 1)
    slot_k = rem(slot, rp)
    have = jnp.where(slot_k < rv, div(slot, rp) * rv + slot_k, -2)
    unpk[...] = (want == have).astype(F32).astype(BF16)

    q_copy.wait()
    for h in range(heads):
        qs[h * bp:h * bp + seqs, :] = qv[:, h * HEAD_DIM:(h + 1) * HEAD_DIM].astype(F32)

    rowl = iota((bp, LANES), 0)
    lane = iota((bp, LANES), 1)
    for c in numbers:
        c.wait()
    mine = jnp.zeros((bp, LANES), F32)
    for t in range(toks):
        for k in range(2):
            mine = mine + jnp.where((rowl == my_e * toks + t) & (lane == k), ids_ref[k, t].astype(F32), 0.0)
    idx[my_e] = mine

    def send(src, dst, send_sem, recv_sem, device):
        c = pltpu.make_async_remote_copy(src, dst, send_sem, recv_sem, device_id=device, device_id_type=MESH)
        c.start()
        return c

    peer = {"seq": to_seq[1 % n_seq], "exp": to_exp[1 % n_exp]}

    def whole(buf, count, sems):
        part = buf.at[pl.ds(0, count)]
        return pltpu.make_async_remote_copy(part, part, sems.at[0], sems.at[1], device_id=peer, device_id_type=MESH)

    def spread(buf, sems, axis, mine_at, to):
        for k in reversed(range(1, len(to))):
            send(buf.at[mine_at], buf.at[mine_at], sems.at[0], sems.at[1], {axis: to[k]})
        return whole(buf, len(to) - 1, sems)

    first = me * span
    pos = iota((heads, span), 1) + first
    hrow = iota((heads, 1), 0)
    kv_of = div(hrow, group)
    diag = div(iota((heads, kvl * HEAD_DIM), 1), HEAD_DIM) == kv_of
    lane_h = iota((heads, LANES), 1)

    def attend(batch):
        scores = []
        for b in batch:
            qb = qs[pl.ds(b, heads, stride=bp), :]
            qd = jnp.where(diag, jnp.concatenate([qb] * kvl, axis=1), 0.0).astype(BF16)
            scores.append(dot_nt(qd, kbuf[b]) * (1.0 / math.sqrt(HEAD_DIM)))
        weights = []
        for b, s in zip(batch, scores):
            live = pos < len_ref[b]
            m = jnp.max(jnp.where(live, s, masked_score), axis=1, keepdims=True).astype(BF16).astype(F32)
            w = jnp.where(live, jnp.exp(s - m), 0.0)
            weights.append((m, jnp.sum(w, axis=1, keepdims=True), w.astype(BF16)))
        for b, (m, l, w) in zip(batch, weights):
            wide = dot(w, vbuf[b])
            acc = jnp.zeros((heads, HEAD_DIM), F32)
            for kv in range(kvl):
                acc = acc + jnp.where(kv_of == kv, wide[:, kv * HEAD_DIM:(kv + 1) * HEAD_DIM], 0.0)
            l_hi = l.astype(BF16).astype(F32)
            at = rem(hrow + b * heads, rv)
            stat = jnp.where(lane_h == at, m, jnp.where(
                lane_h == at + rp, l_hi, jnp.where(lane_h == at + 2 * rp, l - l_hi, 0.0)))
            h0 = 0
            while h0 < heads:
                p, k0 = divmod(b * heads + h0, rv)
                count = min(rv - k0, heads - h0)
                pk[p * rp + k0:p * rp + k0 + count, :] = acc[h0:h0 + count]
                sk[p * rp + k0:p * rp + k0 + count, :] = stat[h0:h0 + count]
                h0 += count

    per = BATCH
    for b0 in range(0, seqs, per):
        batch = range(b0, min(b0 + per, seqs))
        some = pl.ds(b0, len(batch))
        pltpu.make_async_copy(k_hbm.at[some], kbuf.at[some], kv_sem.at[b0 // BATCH, 0]).wait()
        pltpu.make_async_copy(v_hbm.at[some], vbuf.at[some], kv_sem.at[b0 // BATCH, 1]).wait()
        if b0 + per >= seqs:
            for c in small + [ow_copy]:
                c.start()
            for i in waves[0]:
                weight_start(i)
        attend(batch)
    for p in range(n_seq):
        pk[p * rp + rv:p * rp + rv + 1, :] = jnp.sum(sk[p * rp:(p + 1) * rp, :], axis=0, keepdims=True)
    for p in range(n_seq):
        send1[p] = pk[p * rp:(p + 1) * rp, :].astype(BF16)
    recv1[me] = send1[me]
    pl.semaphore_wait(barrier, n - 1)
    for k in reversed(range(1, n_seq)):
        send(send1.at[to_seq[k]], recv1.at[me], sem1.at[0], sem1.at[1], {"seq": to_seq[k]})
    out1 = whole(recv1, n_seq - 1, sem1)
    outi = spread(idx, semi, "exp", my_e, to_exp)
    out1.wait_recv()
    for i in waves[1]:
        weight_start(i)
    for p in range(n_seq):
        sk[p * rp:(p + 1) * rp, :] = recv1[p].astype(F32)
    stats = sk[pl.ds(rv, n_seq, stride=rp), :]
    fade = jnp.exp(stats - jnp.max(stats, axis=0, keepdims=True))
    sums = pltpu.roll(stats, LANES - rp, 1) + pltpu.roll(stats, LANES - 2 * rp, 1)
    den = jnp.sum(sums * fade, axis=0, keepdims=True)
    share = jnp.where(den > 0.0, fade / jnp.where(den > 0.0, den, 1.0), 0.0)
    same = (iota((rp, LANES), 1) == iota((rp, LANES), 0)) & (iota((rp, LANES), 0) < rv)
    att = jnp.zeros((rp, HEAD_DIM), F32)
    for p in range(n_seq):
        col = jnp.sum(jnp.where(same, share[p:p + 1, :], 0.0), axis=1, keepdims=True)
        att = att + sk[p * rp:(p + 1) * rp, :] * col
    buf2[me] = att.astype(BF16)
    out2 = spread(buf2, sem2, "seq", me, to_seq)
    for c in small:
        c.wait()
    ow_copy.wait()
    outi.wait_recv()
    idv = functools.reduce(lambda a, b: a + b, [idx[e] for e in range(n_exp)]).astype(jnp.int32)
    ids = [idv[:, k:k + 1] for k in range(2)]
    rowb = iota((bp, 1), 0)
    place = rem(rowb, toks)
    keep = []
    for k in range(2):
        rank = jnp.zeros((bp, 1), jnp.int32)
        for d in range(1, toks):
            for j in range(2):
                before = pltpu.roll(idv, d, 0)[:, j:j + 1]
                rank = rank + jnp.where((place >= d) & (ids[k] == before), 1, 0)
        limit = jnp.zeros((bp, 1), jnp.int32)
        for e in range(n_experts):
            limit = limit + jnp.where(ids[k] == e, cap_ref[e], 0)
        keep.append((rank < limit) & (rowb < seqs))
    out2.wait_recv()

    rows = dot(unpk[...], jnp.concatenate([buf2[p] for p in range(n_seq)], axis=0))
    att_all = jnp.concatenate([rows[h * bp:(h + 1) * bp] for h in range(heads)], axis=1).astype(BF16)
    part = dot(att_all, ow[...])
    hidden = hid[...].astype(F32)
    rowc = iota((bp, width), 0)
    for t in range(toks):
        part = part + jnp.where(rowc == my_e * toks + t, hidden[t:t + 1, :], 0.0)
    here = me * n_exp + my_e
    buf4[here] = (part * gain[...]).astype(BF16)
    buf3[my_e] = part
    group_size = in_chunk * n_exp
    both_ways = chunks & (chunks - 1) == 0
    for i in range(chunks):
        for at, (to_e, to_s) in enumerate(chunk_members(i)):
            if i or at:
                back = (in_chunk - at // n_exp) % in_chunk * n_exp + (n_exp - at % n_exp) % n_exp
                arrival = group_size + (i if both_ways else chunks - i) if i else back
                send(buf4.at[here], buf4.at[here], sem4.at[0], sem4.at[arrival], {"seq": to_s, "exp": to_e})
        if i == 0:
            out3 = spread(buf3, sem3, "exp", my_e, to_exp)
    out4 = pltpu.make_async_remote_copy(
        buf4.at[pl.ds(0, n - 1)], buf4.at[pl.ds(0, n - 1)], sem4.at[0], sem4.at[1], device_id=peer, device_id_type=MESH)

    half = LANES // 2

    for i in range(chunks):
        if i:
            part = buf4.at[pl.ds(chunk_at[i] * group_size, group_size)]
            pltpu.make_async_remote_copy(
                part, part, sem4.at[0], sem4.at[group_size + i], device_id=peer, device_id_type=MESH).wait_recv()
        else:
            for at, (of_e, of_s) in enumerate(chunk_members(0)):
                if at:
                    part = buf4.at[of_s * n_exp + of_e]
                    pltpu.make_async_remote_copy(
                        part, part, sem4.at[0], sem4.at[at], device_id=peer, device_id_type=MESH).wait_recv()
        if i == chunks - 1:
            outs.wait_recv()
            tot = functools.reduce(lambda a, b: a + b, [st4[p].astype(F32) for p in range(n_seq)])
            tot = tot + pltpu.roll(tot, half, 1)
            scale = lax.rsqrt(tot[:, n_experts:n_experts + 1] / model + norm_eps)
            logits = jnp.where(lane < n_experts, tot, 0.0) * scale
            chosen = [jnp.sum(jnp.where(lane == ids[k], logits, 0.0), axis=1, keepdims=True) for k in range(2)]
            coef = [jnp.where(keep[k], jax.nn.sigmoid(chosen[k] - chosen[1 - k]), 0.0) for k in range(2)]
        if i == 0:
            out3.wait_recv()
        weight_wait(i)
        s = i % slots
        if i == 0:
            residual = functools.reduce(lambda a, b: a + b, [buf3[e] for e in range(n_exp)])
            gained = residual * gain[...]
            top = gained.astype(BF16).astype(F32)
            both = dot_nt(jnp.concatenate([top, gained - top], axis=0).astype(BF16), rt[...])
            pad = jnp.zeros((bp, LANES - n_experts), F32)
            logit = jnp.concatenate([both[:bp] + both[bp:], pad], axis=1)
            square = jnp.sum(residual * residual, axis=1, keepdims=True)
            st = jnp.where(lane == n_experts, square, logit)
            st_hi = st.astype(BF16).astype(F32)
            st4[me] = (st_hi + pltpu.roll(st - st_hi, half, 1)).astype(BF16)
            own = jnp.concatenate([
                jnp.sum(jnp.where(rowc == my_e * toks + t, residual, 0.0), axis=0, keepdims=True) for t in range(toks)
            ], axis=0)
        pieces = []
        for r in range(in_chunk):
            at = chunk_at[i] * in_chunk + r
            pieces.append(functools.reduce(lambda a, b: a + b, [buf4[at * n_exp + e].astype(F32) for e in range(n_exp)]))
        x = jnp.concatenate(pieces, axis=1).astype(BF16)
        for m in range(chunks):
            part = dot(x, pool[s, m * kc:(m + 1) * kc, :])
            gu[m] = part if i == 0 else gu[m] + part
        refill(i)
        if i == 0:
            outs = spread(st4, sems, "seq", me, to_seq)

    inner = []
    for e in range(local):
        ge = my_e * local + e
        c = jnp.where(ids[0] == ge, coef[0], 0.0) + jnp.where(ids[1] == ge, coef[1], 0.0)
        inner.append(jax.nn.silu(gu[2 * e] * scale) * (gu[2 * e + 1] * scale) * c)
    inner = jnp.concatenate(inner, axis=1).astype(BF16)

    for i in range(local):
        weight_wait(chunks + i)
        s = (chunks + i) % slots
        deep = local * ffl
        y = jnp.concatenate(
            [dot(inner, pool[s, j * deep:(j + 1) * deep, :]) for j in range(cols // ffl)], axis=1).astype(BF16)
        base = block_at[i] * in_block
        for e in range(n_exp):
            for r in range(in_block):
                ysend[e * n_seq + base + r] = y[e * toks:(e + 1) * toks, r * width:(r + 1) * width]
        refill(chunks + i)
        for r in range(in_block):
            for k in range(n_exp):
                to_s = base + lax.rem(block_pos + r, in_block)
                to = to_exp[k] * n_seq + to_s
                if i == local - 1 and r == 0 and k == 0:
                    yrecv[me_all] = ysend[me_all]
                else:
                    send(ysend.at[to], yrecv.at[me_all], sem5.at[0], sem5.at[1], {"seq": to_s, "exp": to_exp[k]})
    out5 = whole(yrecv, n - 1, sem5)
    for c in (out1, outi, out2, out3, out4, outs):
        c.wait_send()
    total = own
    out5.wait_recv()
    for p in range(n):
        total = total + yrecv[p].astype(F32)
    o_ref[...] = total.astype(BF16)
    out5.wait_send()


def on_device(
    n_seq, n_exp, hidden_in, queries, key_cache, value_cache, lengths, out_weight, norm_gain,
    router, expert_ids, capacity, w_gate, w_up, w_down,
):
    seqs = queries.shape[0]
    toks, width = hidden_in.shape
    span, kv_width = key_cache.shape[1:]
    kvl = kv_width // HEAD_DIM
    heads = queries.shape[1] // HEAD_DIM
    group = heads // kvl
    bp = up(seqs, 8)
    n_experts = router.shape[1]
    model = width * n_seq
    local, _, ffl = w_gate.shape
    rv = -(-seqs * heads // n_seq)
    rp = up(rv + 1, 16)
    n = n_seq * n_exp
    fixed = 2 * (2 * seqs * span * kv_width + out_weight.size)
    spare = 7 << 18
    slots = min(3 * local, (VMEM_BYTES - fixed - spare) // (2 * model * ffl))
    vmem = pl.BlockSpec(memory_space=pltpu.VMEM)
    hbm = pl.BlockSpec(memory_space=pltpu.HBM)
    dma = pltpu.SemaphoreType.DMA
    return pl.pallas_call(
        functools.partial(layer_kernel, (n_seq, n_exp, seqs, toks, kvl, group, rv, rp, n_experts, slots)),
        in_specs=[hbm] * 13,
        out_specs=vmem,
        out_shape=pltpu.VMEM((toks, width), BF16),
        scratch_shapes=[
            pltpu.SMEM(lengths.shape, jnp.int32),
            pltpu.SMEM(capacity.shape, jnp.int32),
            pltpu.SMEM(expert_ids.shape[::-1], jnp.int32),
            pltpu.VMEM((toks, width), BF16),
            pltpu.VMEM(queries.shape, BF16),
            pltpu.VMEM(key_cache.shape, BF16),
            pltpu.VMEM(value_cache.shape, BF16),
            pltpu.VMEM(out_weight.shape, BF16),
            pltpu.VMEM((1, width), F32),
            pltpu.VMEM((n_experts, width), BF16),
            pltpu.VMEM((slots, model, ffl), BF16),
            pltpu.VMEM((heads * bp, HEAD_DIM), F32),
            pltpu.VMEM((n_seq * rp, HEAD_DIM), F32),
            pltpu.VMEM((n_seq * rp, HEAD_DIM), F32),
            pltpu.VMEM((heads * bp, n_seq * rp), BF16),
            pltpu.VMEM((n_seq, rp, HEAD_DIM), BF16),
            pltpu.VMEM((n_seq, rp, HEAD_DIM), BF16),
            pltpu.VMEM((n_seq, rp, HEAD_DIM), BF16),
            pltpu.VMEM((n_exp, bp, width), F32),
            pltpu.VMEM((n_exp, bp, LANES), F32),
            pltpu.VMEM((n, bp, width), BF16),
            pltpu.VMEM((n_seq, bp, LANES), BF16),
            pltpu.VMEM((2 * local, bp, ffl), F32),
            pltpu.VMEM((n, toks, width), BF16),
            pltpu.VMEM((n, toks, width), BF16),
            dma((8,)), dma((-(-seqs // BATCH), 2)), dma((3 * local,)),
            dma((2,)), dma((2,)), dma((2,)), dma((2,)), dma((n // (2 * local) + 2 * local,)), dma((2,)), dma((2,)),
        ],
        compiler_params=pltpu.CompilerParams(
            collective_id=0, has_side_effects=True, vmem_limit_bytes=VMEM_BYTES),
        name="layer",
    )(
        lengths, capacity, expert_ids.T, hidden_in, queries, key_cache, value_cache, out_weight, norm_gain,
        router.T, w_gate, w_up, w_down,
    )


def solution(mesh):
    in_specs = (
        P("exp", "seq"),
        P(None, "exp"),
        P(None, "seq", "exp"),
        P(None, "seq", "exp"),
        P(),
        P("exp", "seq"),
        P("seq"),
        P("seq", None),
        P("exp", None),
        P(),
        P("exp", None, "seq"),
        P("exp", None, "seq"),
        P("exp", "seq", None),
    )
    return jax.shard_map(
        functools.partial(on_device, mesh.shape["seq"], mesh.shape["exp"]),
        mesh=mesh, in_specs=in_specs, out_specs=P("exp", "seq"), check_vma=False,
    )
```
